32 devices in a mesh: pair: 4 (over y, x), virt: 8 (over z, core).
Axes of the slice: x: 2, y: 2, z: 4, core: 2. Of those that a mesh axis runs over, the one named last changes fastest.
Arguments:
- density_row_blocks: bfloat16 [160, 128, 2744], P('pair', 'virt'), may hold values from -6 to 6
- vir_left: bfloat16 [128, 2744], P('virt'), may hold values from -0.046875 to 0.046875
- vir_right: bfloat16 [128, 2744], P('virt'), may hold values from -0.109375 to 0.109375
- orb_energy: bfloat16 [128], P('virt'), may hold values from 0.5 to 3
- state_energy: float32 [8], replicated, may hold values from -1 to -0.1
- bra_ket_states: int32 [160, 2], P('pair'), may hold values from 0 to 7
- row_block_starts: int32 [160], P('pair'), may hold values from 0 to 2616
Outputs:
- slot_couplings: float32 [160], P('pair')
- heff: float32 [8, 8], replicated
The draws below stay inside these ranges and needn't reach their ends.
All inputs are finite; a program needn't handle non-finite values.
Results may differ from the reference program's by a relative error of at most 0.0003.
Values may be sent and summed in bfloat16 or wider, within the bound.
A program may use at most 64 MiB of HBM per device.

```python
import jax
import jax.numpy as jnp
from jax import lax

MODEL_STATES = 8
ACTIVE_TRIPLES = 2744
NV = 128
BLOCK_ROW_COUNT = 128
DENSITY_BLOCKS = 160


def touch_ends(entries, stream_key, least, largest):
    longest = entries.shape.index(max(entries.shape))
    spots = []
    for shift in (0, 1):
        where = [jax.random.randint(jax.random.fold_in(stream_key, axis), (), 0, length) for axis, length in enumerate(entries.shape)]
        where[longest] = (where[longest] + shift) % entries.shape[longest]
        spots.append(tuple(where))
    return entries.at[spots[0]].set(least).at[spots[1]].set(largest)


def levels(own_key, shape, shards, low, largest):
    factor_of, own = 1.0, jax.random.fold_in(own_key, 6)
    for axis_at, blocks in shards:
        heights = jnp.exp(jax.random.uniform(jax.random.fold_in(own, axis_at), (blocks,), jnp.float32, low / len(shards), largest / len(shards)))
        factor_of = factor_of * jnp.repeat(heights, shape[axis_at] // blocks).reshape([-1 if axis == axis_at else 1 for axis in range(len(shape))])
    return factor_of


def normal_values(own_key, shape, spread, bound, shards=(), kind=jnp.bfloat16):
    drawn = jax.random.normal(own_key, shape, jnp.float32) * spread
    if len(shards) > 0:
        drawn = levels(own_key, shape, shards, -0.22, 0.18) * drawn
    return jnp.clip(drawn, min=-bound, max=bound).astype(kind)


def setup_inputs(seed: int = 0) -> dict:
    arg_keys = jax.random.split(jax.random.key(seed), 8)
    density_row_blocks = normal_values(arg_keys[0], (DENSITY_BLOCKS, BLOCK_ROW_COUNT, ACTIVE_TRIPLES), 1.0, 6.0, ((0, 4), (1, 8)))
    vir_left = normal_values(arg_keys[1], (NV, ACTIVE_TRIPLES), (BLOCK_ROW_COUNT * NV) ** -0.5, 0.046875, ((0, 8),))
    vir_right = normal_values(arg_keys[2], (NV, ACTIVE_TRIPLES), ACTIVE_TRIPLES ** -0.5, 0.109375, ((0, 8),))
    orb_energy = jnp.clip(0.5 + 2.5 * jax.random.uniform(arg_keys[3], (NV,), jnp.float32) ** levels(arg_keys[3], (NV,), ((0, 8),), -0.2, 0.2), 0.5, 3.0).astype(jnp.bfloat16)
    state_energy = jnp.clip(jax.random.uniform(arg_keys[4], (MODEL_STATES,), jnp.float32, -1.0, -0.1), -1.0, -0.1)
    bra_ket_states = touch_ends(jax.random.randint(arg_keys[5], (DENSITY_BLOCKS, 2), 0, MODEL_STATES), jax.random.fold_in(arg_keys[5], 1), 0, MODEL_STATES - 1).astype(jnp.int32)
    row_block_starts = touch_ends(jax.random.randint(arg_keys[6], (DENSITY_BLOCKS,), 0, ACTIVE_TRIPLES - BLOCK_ROW_COUNT + 1), jax.random.fold_in(arg_keys[6], 1), 0, ACTIVE_TRIPLES - BLOCK_ROW_COUNT).astype(jnp.int32)
    return dict(density_row_blocks=density_row_blocks, vir_left=vir_left, vir_right=vir_right, orb_energy=orb_energy, state_energy=state_energy, bra_ket_states=bra_ket_states, row_block_starts=row_block_starts)


def reference(density_row_blocks, vir_left, vir_right, orb_energy, state_energy, bra_ket_states, row_block_starts):
    block_rows = density_row_blocks.shape[1]
    energy = orb_energy.astype(jnp.float32)

    def single(items):
        block, couple, offset = items
        columns = lax.dynamic_slice_in_dim(vir_left, offset.astype(jnp.int32), block_rows, 1)
        contracted = jnp.dot(vir_right, block.T, preferred_element_type=jnp.float32)
        shift = state_energy[couple[0]] + state_energy[couple[1]]
        inverse = 1.0 / (energy - shift)
        return jnp.sum(columns.astype(jnp.float32) * contracted * inverse[:, None])

    couplings = lax.map(single, (density_row_blocks, bra_ket_states, row_block_starts))
    states = jnp.arange(MODEL_STATES, dtype=jnp.int32)
    first = (bra_ket_states[:, 0:1] == states[None, :]).astype(jnp.float32)
    second = (bra_ket_states[:, 1:2] == states[None, :]).astype(jnp.float32)
    coupling_sum = jnp.dot(first.T, couplings[:, None] * second, precision=lax.Precision.HIGHEST)
    heff = jnp.diag(state_energy) + 0.5 * (coupling_sum + coupling_sum.T)
    return couplings, heff
```

```python
import functools

import jax
import jax.numpy as jnp
from jax import lax
from jax.experimental import pallas as pl
from jax.experimental.pallas import tpu as pltpu
from jax.sharding import PartitionSpec as P

MESH = pl.DeviceIdType.MESH
LANES = 128


def windows(
    l_raw,
    e_ref,
    se_ref,
    states_ref,
    starts_ref,
    w_send,
    shift_ref,
    bra_ref,
    ket_ref,
    l_f32,
):
    nvirt, avirt, _ = w_send.shape
    ntrip = l_raw.shape[1]
    slots = starts_ref.shape[0]
    rows = shift_ref.shape[1] // slots
    group = LANES // rows
    blocks = slots // group

    l_f32[...] = jnp.zeros_like(l_f32)
    l_f32[:, :ntrip] = l_raw[...].astype(jnp.float32)
    lane = lax.broadcasted_iota(jnp.int32, (avirt, LANES), 1) // rows
    width = rows * nvirt
    load_width = width + LANES

    def window_block(b, carry):
        views = []
        for j in range(group):
            offset = starts_ref[b * group + j]
            rest = offset % LANES
            base = pl.multiple_of(offset - rest, LANES)
            wide = l_f32[:, pl.ds(base, load_width)]
            turned = pltpu.roll(wide, (load_width - rest) % load_width, 1)
            views.append(turned[:, :width])
        for q in range(nvirt // group):
            held = [v[:, q * LANES : (q + 1) * LANES] for v in views]
            bit = 1
            while bit < group:
                keep = (lane & bit) == 0
                fresh = list(held)
                for j in range(group):
                    if j & bit == 0:
                        a, o = held[j], held[j | bit]
                        fresh[j] = jnp.where(keep, a, pltpu.roll(o, bit * rows, 1))
                        fresh[j | bit] = jnp.where(keep, pltpu.roll(a, LANES - bit * rows, 1), o)
                held = fresh
                bit *= 2
            for i in range(group):
                w_send[q * group + i, :, pl.ds(pl.multiple_of(b * LANES, LANES), LANES)] = held[
                    i
                ].astype(jnp.bfloat16)
        return carry

    lax.fori_loop(0, blocks, window_block, 0)
    square = (
        lax.broadcasted_iota(jnp.int32, (avirt, avirt), 0)
        == lax.broadcasted_iota(jnp.int32, (avirt, avirt), 1)
    )
    energy_own = jnp.sum(
        jnp.where(square, e_ref[...].astype(jnp.float32), 0.0), axis=1, keepdims=True
    )
    energy_own = jnp.broadcast_to(energy_own, (avirt, LANES)).astype(jnp.bfloat16)
    for i in range(nvirt):
        w_send[i, :, blocks * LANES :] = energy_own

    wide_lane = lax.broadcasted_iota(jnp.int32, (1, LANES), 1)
    bra = jnp.full((1, LANES), -1, jnp.int32)
    ket = jnp.full((1, LANES), -1, jnp.int32)
    shifts = []
    for b in range(blocks):
        shift = jnp.zeros((1, LANES), jnp.float32)
        for j in range(group):
            s = b * group + j
            i_state, j_state = states_ref[s], states_ref[slots + s]
            total = se_ref[i_state] + se_ref[j_state]
            shift = jnp.where(wide_lane // rows == j, total, shift)
            bra = jnp.where(wide_lane == s, i_state, bra)
            ket = jnp.where(wide_lane == s, j_state, ket)
        shifts.append(shift)
    shift_ref[...] = jnp.concatenate(shifts, axis=1)
    bra_ref[...] = bra
    ket_ref[...] = ket


def kernel(
    npair,
    nvirt,
    chunks,
    d_hbm,
    r_hbm,
    w_send,
    shift_ref,
    bra_ref,
    ket_ref,
    se_ref,
    coup_ref,
    heff_ref,
    d_all,
    r_all,
    w_all,
    p_send,
    p_all,
    h_send,
    h_all,
    d_sem,
    o_sem,
    own_sem,
    r_ssem,
    r_rsem,
    f_ssem,
    w_ssem,
    w_rsem,
    p_ssem,
    p_rsem,
    h_ssem,
    h_rsem,
):
    slots, rows, ntrip = d_all.shape
    nstate = heff_ref.shape[0]
    avirt = r_all.shape[1]
    nz = nvirt // 2
    group = LANES // rows
    blocks = slots // group
    me = lax.axis_index("virt")
    my_pair = lax.axis_index("pair")
    my_z, my_c = me // 2, me % 2
    sibling = my_z * 2 + 1 - my_c
    z_order = sorted(range(1, nz), key=lambda d: -min(d, nz - d))

    r_copy = pltpu.make_async_copy(r_hbm, r_all.at[me], o_sem)
    r_copy.start()
    d_copy = pltpu.make_async_copy(d_hbm, d_all, d_sem)
    d_copy.start()

    barrier = pltpu.get_barrier_semaphore()
    for k in range(1, nvirt):
        pl.semaphore_signal(
            barrier, inc=1, device_id={"virt": (me + k) % nvirt}, device_id_type=MESH
        )
    for k in range(1, npair):
        pl.semaphore_signal(
            barrier, inc=1, device_id={"pair": (my_pair + k) % npair}, device_id_type=MESH
        )
    pl.semaphore_wait(barrier, nvirt + npair - 2)

    r_copy.wait()

    def piece(source, c):
        lo, width = chunks[c]
        return r_all.at[source, :, pl.ds(lo, width)]

    def send_right(source, c, target, send_sem):
        return pltpu.make_async_remote_copy(
            src_ref=piece(source, c),
            dst_ref=piece(source, c),
            send_sem=send_sem,
            recv_sem=r_rsem.at[source, c],
            device_id={"virt": target},
            device_id_type=MESH,
        )

    sends = []
    for c in range(len(chunks)):
        for n, dz in enumerate(z_order):
            target = ((my_z + dz) % nz) * 2 + my_c
            sends.append(send_right(me, c, target, r_ssem.at[n, c]))
            sends[-1].start()
        sends.append(send_right(me, c, sibling, r_ssem.at[nz - 1, c]))
        sends[-1].start()

    def send_window(k):
        target = (me + k) % nvirt
        return pltpu.make_async_remote_copy(
            src_ref=w_send.at[target],
            dst_ref=w_all.at[me],
            send_sem=w_ssem.at[k],
            recv_sem=w_rsem.at[me],
            device_id={"virt": target},
            device_id_type=MESH,
        )

    for k in range(1, nvirt):
        sends.append(send_window(k))
        sends[-1].start()
    own = pltpu.make_async_copy(w_send.at[me], w_all.at[me], own_sem)
    own.start()

    for c in range(len(chunks)):
        for dz in range(1, nz):
            source = ((my_z + dz) % nz) * 2 + my_c
            send_right(source, c, sibling, f_ssem.at[dz, c]).wait_recv()
            forward = send_right(source, c, sibling, f_ssem.at[dz, c])
            forward.start()
            sends.append(forward)
    d_copy.wait()
    total = None
    for c, (lo, cw) in enumerate(chunks):
        for dz in range(nz):
            source = ((my_z + dz) % nz) * 2 + 1 - my_c
            send_right(source, c, sibling, f_ssem.at[0, c]).wait_recv()
        part = lax.dot_general(
            r_all[:, :, lo : lo + cw].reshape(nvirt * avirt, cw),
            d_all[:, :, lo : lo + cw].reshape(slots * rows, cw),
            (((1,), (1,)), ((), ())),
            preferred_element_type=jnp.float32,
        )
        total = part if total is None else total + part
    own.wait()
    for k in range(1, nvirt):
        source = (me + k) % nvirt
        pltpu.make_async_remote_copy(
            src_ref=w_send.at[source],
            dst_ref=w_all.at[source],
            send_sem=w_ssem.at[0],
            recv_sem=w_rsem.at[source],
            device_id={"virt": source},
            device_id_type=MESH,
        ).wait_recv()
    columns = w_all[:, :, : blocks * LANES].reshape(nvirt * avirt, blocks * LANES)
    energy = w_all[:, :, blocks * LANES :].reshape(nvirt * avirt, LANES)[:, :1]
    inverse = 1.0 / (energy.astype(jnp.float32) - shift_ref[...])
    summed = jnp.sum(total * columns.astype(jnp.float32) * inverse, axis=0, keepdims=True)
    gather_lanes = (
        lax.broadcasted_iota(jnp.int32, (slots * rows, LANES), 0) // rows
        == lax.broadcasted_iota(jnp.int32, (slots * rows, LANES), 1)
    ).astype(jnp.float32)
    partial = jnp.dot(
        jnp.broadcast_to(summed, (8, slots * rows)),
        gather_lanes,
        precision=lax.Precision.HIGHEST,
        preferred_element_type=jnp.float32,
    )[:1]

    p_send[...] = partial
    for k in range(1, nvirt):
        target = (me + k) % nvirt
        sends.append(
            pltpu.make_async_remote_copy(
                src_ref=p_send,
                dst_ref=p_all.at[me],
                send_sem=p_ssem.at[k],
                recv_sem=p_rsem.at[me],
                device_id={"virt": target},
                device_id_type=MESH,
            )
        )
        sends[-1].start()
    p_all[me] = partial
    for k in range(1, nvirt):
        source = (me + k) % nvirt
        pltpu.make_async_remote_copy(
            src_ref=p_send,
            dst_ref=p_all.at[source],
            send_sem=p_ssem.at[0],
            recv_sem=p_rsem.at[source],
            device_id={"virt": source},
            device_id_type=MESH,
        ).wait_recv()
    couplings = jnp.sum(p_all[...], axis=0)
    coup_ref[...] = couplings[:, :slots]

    row = lax.broadcasted_iota(jnp.int32, (nstate, LANES), 0)
    first = (row == bra_ref[...]).astype(jnp.float32)
    second = (row == ket_ref[...]).astype(jnp.float32)
    over_lanes = (((1,), (1,)), ((), ()))
    direct = lax.dot_general(
        first * couplings, second, over_lanes, precision=lax.Precision.HIGHEST,
        preferred_element_type=jnp.float32,
    )
    turned = lax.dot_general(
        second * couplings, first, over_lanes, precision=lax.Precision.HIGHEST,
        preferred_element_type=jnp.float32,
    )
    both = direct + turned
    h_send[...] = jnp.concatenate(
        [both, jnp.zeros((nstate, LANES - nstate), jnp.float32)], axis=1
    )
    for k in range(1, npair):
        target = (my_pair + k) % npair
        sends.append(
            pltpu.make_async_remote_copy(
                src_ref=h_send,
                dst_ref=h_all.at[my_pair],
                send_sem=h_ssem.at[k],
                recv_sem=h_rsem.at[my_pair],
                device_id={"pair": target},
                device_id_type=MESH,
            )
        )
        sends[-1].start()
    h_all[my_pair] = h_send[...]
    si = lax.broadcasted_iota(jnp.int32, (nstate, nstate), 0)
    sj = lax.broadcasted_iota(jnp.int32, (nstate, nstate), 1)
    diagonal = jnp.zeros((nstate, nstate), jnp.float32)
    for n in range(nstate):
        diagonal = jnp.where((si == n) & (sj == n), se_ref[n], diagonal)
    for k in range(1, npair):
        source = (my_pair + k) % npair
        pltpu.make_async_remote_copy(
            src_ref=h_send,
            dst_ref=h_all.at[source],
            send_sem=h_ssem.at[0],
            recv_sem=h_rsem.at[source],
            device_id={"pair": source},
            device_id_type=MESH,
        ).wait_recv()
    heff_ref[...] = diagonal + 0.5 * jnp.sum(h_all[...], axis=0)[:, :nstate]
    for send in sends:
        send.wait_send()


def local(
    npair,
    nvirt,
    density_row_blocks,
    vir_left,
    vir_right,
    orb_energy,
    state_energy,
    bra_ket_states,
    row_block_starts,
):
    slots, rows, ntrip = density_row_blocks.shape
    avirt = vir_left.shape[0]
    nstate = state_energy.shape[0]
    padded = -(-ntrip // LANES) * LANES
    half = -(-(padded // LANES) // 2) * LANES
    chunks = ((0, half), (half, ntrip - half))
    nch = len(chunks)
    wide = slots * rows + LANES
    any_space = pl.BlockSpec(memory_space=pltpu.HBM)
    vmem = pl.BlockSpec(memory_space=pltpu.VMEM)
    smem = pl.BlockSpec(memory_space=pltpu.SMEM)
    dma = pltpu.SemaphoreType.DMA
    w_send, shift, bra, ket = pl.pallas_call(
        windows,
        out_shape=(
            jax.ShapeDtypeStruct((nvirt, avirt, wide), jnp.bfloat16),
            jax.ShapeDtypeStruct((1, slots * rows), jnp.float32),
            jax.ShapeDtypeStruct((1, LANES), jnp.int32),
            jax.ShapeDtypeStruct((1, LANES), jnp.int32),
        ),
        in_specs=[vmem, vmem, smem, smem, smem],
        out_specs=(vmem,) * 4,
        scratch_shapes=[pltpu.VMEM((avirt, padded + nvirt * rows), jnp.float32)],
    )(
        vir_left,
        orb_energy.reshape(1, avirt),
        state_energy,
        bra_ket_states.T.reshape(2 * slots),
        row_block_starts,
    )
    couplings, heff = pl.pallas_call(
        functools.partial(kernel, npair, nvirt, chunks),
        out_shape=(
            jax.ShapeDtypeStruct((1, slots), jnp.float32),
            jax.ShapeDtypeStruct((nstate, nstate), jnp.float32),
        ),
        in_specs=[any_space, any_space, vmem, vmem, vmem, vmem, smem],
        out_specs=(vmem, vmem),
        scratch_shapes=[
            pltpu.VMEM((slots, rows, ntrip), jnp.bfloat16),
            pltpu.VMEM((nvirt, avirt, ntrip), jnp.bfloat16),
            pltpu.VMEM((nvirt, avirt, wide), jnp.bfloat16),
            pltpu.VMEM((1, LANES), jnp.float32),
            pltpu.VMEM((nvirt, 1, LANES), jnp.float32),
            pltpu.VMEM((nstate, LANES), jnp.float32),
            pltpu.VMEM((npair, nstate, LANES), jnp.float32),
            dma,
            dma,
            dma,
            dma((nvirt // 2, nch)),
            dma((nvirt, nch)),
            dma((nvirt // 2, nch)),
            dma((nvirt,)),
            dma((nvirt,)),
            dma((nvirt,)),
            dma((nvirt,)),
            dma((npair,)),
            dma((npair,)),
        ],
        compiler_params=pltpu.CompilerParams(
            collective_id=0, has_side_effects=True, vmem_limit_bytes=60 * 1024 * 1024
        ),
    )(
        density_row_blocks,
        vir_right,
        w_send,
        shift,
        bra,
        ket,
        state_energy,
    )
    return couplings.reshape(slots), heff


def solution(mesh):
    npair, nvirt = mesh.shape["pair"], mesh.shape["virt"]
    placed = (
        P("pair", "virt", None),
        P("virt", None),
        P("virt", None),
        P("virt"),
        P(),
        P("pair", None),
        P("pair"),
    )
    return jax.shard_map(
        functools.partial(local, npair, nvirt),
        mesh=mesh,
        in_specs=placed,
        out_specs=(P("pair"), P()),
        check_vma=False,
    )
```

```python
import functools

import jax
import jax.numpy as jnp
from jax import lax
from jax.experimental import pallas as pl
from jax.experimental.pallas import tpu as pltpu
from jax.sharding import PartitionSpec as P

MESH = pl.DeviceIdType.MESH
LANES = 128


def windows(
    l_raw,
    r_raw,
    e_ref,
    se_ref,
    states_ref,
    starts_ref,
    w_send,
    r_own,
    shift_ref,
    place_ref,
    l_f32,
):
    nvirt, avirt, _ = w_send.shape
    ntrip = l_raw.shape[1]
    slots = starts_ref.shape[0]
    rows = shift_ref.shape[1] // slots
    group = LANES // rows
    blocks = slots // group

    l_f32[...] = jnp.zeros_like(l_f32)
    l_f32[:, :ntrip] = l_raw[...].astype(jnp.float32)
    lane = lax.broadcasted_iota(jnp.int32, (avirt, LANES), 1) // rows
    width = rows * nvirt
    load_width = width + LANES

    def window_block(b, carry):
        views = []
        for j in range(group):
            offset = starts_ref[b * group + j]
            rest = offset % LANES
            base = pl.multiple_of(offset - rest, LANES)
            wide = l_f32[:, pl.ds(base, load_width)]
            turned = pltpu.roll(wide, (load_width - rest) % load_width, 1)
            views.append(turned[:, :width])
        for q in range(nvirt // group):
            held = [v[:, q * LANES : (q + 1) * LANES] for v in views]
            bit = 1
            while bit < group:
                keep = (lane & bit) == 0
                fresh = list(held)
                for j in range(group):
                    if j & bit == 0:
                        a, o = held[j], held[j | bit]
                        fresh[j] = jnp.where(keep, a, pltpu.roll(o, bit * rows, 1))
                        fresh[j | bit] = jnp.where(keep, pltpu.roll(a, LANES - bit * rows, 1), o)
                held = fresh
                bit *= 2
            for i in range(group):
                w_send[q * group + i, :, pl.ds(pl.multiple_of(b * LANES, LANES), LANES)] = held[
                    i
                ].astype(jnp.bfloat16)
        return carry

    lax.fori_loop(0, blocks, window_block, 0)
    square = (
        lax.broadcasted_iota(jnp.int32, (avirt, avirt), 0)
        == lax.broadcasted_iota(jnp.int32, (avirt, avirt), 1)
    )
    energy_own = jnp.sum(
        jnp.where(square, e_ref[...].astype(jnp.float32), 0.0), axis=1, keepdims=True
    )
    half = r_own.shape[2]
    rest = ntrip - half
    r_own[0] = r_raw[:, :half]
    r_own[1] = jnp.concatenate(
        [r_raw[:, half:], jnp.broadcast_to(energy_own, (avirt, half - rest)).astype(jnp.bfloat16)],
        axis=1,
    )

    wide_lane = lax.broadcasted_iota(jnp.int32, (1, LANES), 1)
    lane_of = lax.broadcasted_iota(jnp.int32, (rows, LANES), 1)
    nstate = se_ref.shape[0]
    shifts = []
    for b in range(blocks):
        shift = jnp.zeros((1, LANES), jnp.float32)
        for j in range(group):
            s = b * group + j
            i_state, j_state = states_ref[0, s], states_ref[1, s]
            total = se_ref[i_state] + se_ref[j_state]
            shift = jnp.where(wide_lane // rows == j, total, shift)
            code = LANES // 2 + i_state * nstate + j_state
            place_ref[s * rows : (s + 1) * rows, :] = (
                ((lane_of == s) | (lane_of == code)).astype(jnp.float32).astype(jnp.bfloat16)
            )
        shifts.append(shift)
    shift_ref[...] = jnp.concatenate(shifts, axis=1)


def kernel(
    npair,
    nvirt,
    d_hbm,
    w_send,
    r_own,
    shift_ref,
    place_ref,
    out_ref,
    d_all,
    r_all,
    w_all,
    p_send,
    p_all,
    h_send,
    h_all,
    d_sem,
    o_sem,
    own_sem,
    z_ssem,
    b_ssem,
    x_ssem,
    f_ssem,
    r_rsem,
    w_ssem,
    w_rsem,
    p_ssem,
    p_rsem,
    h_ssem,
    h_rsem,
):
    slots, rows, ntrip = d_all.shape
    _, _, avirt, half = r_all.shape
    rest = ntrip - half
    nz = nvirt // 2
    me = lax.axis_index("virt")
    my_pair = lax.axis_index("pair")
    my_z, my_c = me // 2, me % 2
    sibling = my_z * 2 + 1 - my_c
    mine = my_pair % 2
    partner = my_pair + 1 - 2 * mine
    z_order = sorted(range(1, nz), key=lambda d: -min(d, nz - d))

    r_copies = [
        pltpu.make_async_copy(r_own.at[h], r_all.at[h, me], o_sem.at[h]) for h in range(2)
    ]
    for copy in r_copies:
        copy.start()
    d_copy = pltpu.make_async_copy(d_hbm, d_all, d_sem)
    d_copy.start()

    barrier = pltpu.get_barrier_semaphore()
    for k in range(1, nvirt):
        pl.semaphore_signal(
            barrier, inc=1, device_id={"virt": (me + k) % nvirt}, device_id_type=MESH
        )
    for k in range(1, npair):
        pl.semaphore_signal(
            barrier, inc=1, device_id={"pair": (my_pair + k) % npair}, device_id_type=MESH
        )
    pl.semaphore_wait(barrier, nvirt + npair - 2)

    def send_right(h, source, device, send_sem, own=False):
        return pltpu.make_async_remote_copy(
            src_ref=r_own.at[h] if own else r_all.at[h, source],
            dst_ref=r_all.at[h, source],
            send_sem=send_sem,
            recv_sem=r_rsem.at[h, source],
            device_id=device,
            device_id_type=MESH,
        )

    sends = []

    def go(copy):
        copy.start()
        sends.append(copy)

    def same_core(dz):
        return ((my_z + dz) % nz) * 2 + my_c

    for dz in z_order:
        go(send_right(mine, me, {"virt": same_core(dz)}, z_ssem.at[dz], True))
    for h in range(2):
        go(send_right(h, me, {"virt": sibling}, b_ssem.at[h], True))
    for k in [2 * dz + o for dz in z_order for o in (0, 1)] + [1]:
        target = (me + k) % nvirt
        go(
            pltpu.make_async_remote_copy(
                src_ref=w_send.at[target],
                dst_ref=w_all.at[me],
                send_sem=w_ssem.at[k],
                recv_sem=w_rsem.at[me],
                device_id={"virt": target},
                device_id_type=MESH,
            )
        )
    own = pltpu.make_async_copy(w_send.at[me], w_all.at[me], own_sem)
    own.start()

    z_near = z_order[::-1]
    for dz in z_near:
        source = same_core(dz)
        send_right(mine, source, {"virt": sibling}, f_ssem.at[0, dz]).wait_recv()
        go(send_right(mine, source, {"pair": partner}, x_ssem.at[dz]))
        go(send_right(mine, source, {"virt": sibling}, f_ssem.at[0, dz]))
    for dz in z_near:
        source = same_core(dz)
        send_right(1 - mine, source, {"virt": sibling}, f_ssem.at[1, dz]).wait_recv()
        go(send_right(1 - mine, source, {"virt": sibling}, f_ssem.at[1, dz]))
    d_copy.wait()
    for copy in r_copies:
        copy.wait()
    for dz in range(nz):
        source = ((my_z + dz) % nz) * 2 + 1 - my_c
        for h in range(2):
            send_right(h, source, {"virt": sibling}, f_ssem.at[0, 0]).wait_recv()
    total = None
    for h, (lo, cw) in enumerate(((0, half), (half, rest))):
        part = lax.dot_general(
            r_all[h, :, :, :cw].reshape(nvirt * avirt, cw),
            d_all[:, :, lo : lo + cw].reshape(slots * rows, cw),
            (((1,), (1,)), ((), ())),
            preferred_element_type=jnp.float32,
        )
        total = part if total is None else total + part
    energy = r_all[1, :, :, half - LANES :].reshape(nvirt * avirt, LANES)[:, LANES - 1 :]
    inverse = 1.0 / (energy.astype(jnp.float32) - shift_ref[...])
    total = total * inverse
    own.wait()
    for k in range(1, nvirt):
        source = (me + k) % nvirt
        pltpu.make_async_remote_copy(
            src_ref=w_send.at[source],
            dst_ref=w_all.at[source],
            send_sem=w_ssem.at[0],
            recv_sem=w_rsem.at[source],
            device_id={"virt": source},
            device_id_type=MESH,
        ).wait_recv()
    columns = w_all[...].reshape(nvirt * avirt, slots * rows)
    summed = jnp.sum(total * columns.astype(jnp.float32), axis=0, keepdims=True)
    high = summed.astype(jnp.bfloat16).astype(jnp.float32)
    middle = (summed - high).astype(jnp.bfloat16).astype(jnp.float32)
    low = summed - high - middle
    terms = jnp.concatenate(
        [high, middle, low, jnp.zeros((5, slots * rows), jnp.float32)], axis=0
    ).astype(jnp.bfloat16)
    placed = jnp.dot(terms, place_ref[...], preferred_element_type=jnp.float32)
    partial = jnp.sum(placed, axis=0, keepdims=True)

    p_send[...] = partial
    for k in list(range(1, nvirt))[::-1]:
        target = (me + k) % nvirt
        go(
            pltpu.make_async_remote_copy(
                src_ref=p_send,
                dst_ref=p_all.at[me],
                send_sem=p_ssem.at[k],
                recv_sem=p_rsem.at[me],
                device_id={"virt": target},
                device_id_type=MESH,
            )
        )
    p_all[me] = partial
    for k in range(1, nvirt):
        source = (me + k) % nvirt
        pltpu.make_async_remote_copy(
            src_ref=p_send,
            dst_ref=p_all.at[source],
            send_sem=p_ssem.at[0],
            recv_sem=p_rsem.at[source],
            device_id={"virt": source},
            device_id_type=MESH,
        ).wait_recv()
    along = jnp.sum(p_all[...], axis=0)
    h_send[...] = along
    for k in range(1, npair):
        target = (my_pair + k) % npair
        go(
            pltpu.make_async_remote_copy(
                src_ref=h_send,
                dst_ref=h_all.at[my_pair],
                send_sem=h_ssem.at[k],
                recv_sem=h_rsem.at[my_pair],
                device_id={"pair": target},
                device_id_type=MESH,
            )
        )
    h_all[my_pair] = along
    for k in range(1, npair):
        source = (my_pair + k) % npair
        pltpu.make_async_remote_copy(
            src_ref=h_send,
            dst_ref=h_all.at[source],
            send_sem=h_ssem.at[0],
            recv_sem=h_rsem.at[source],
            device_id={"pair": source},
            device_id_type=MESH,
        ).wait_recv()
    lane = lax.broadcasted_iota(jnp.int32, (1, LANES), 1)
    out_ref[...] = jnp.where(lane < LANES // 2, along, jnp.sum(h_all[...], axis=0))
    for send in sends:
        send.wait_send()


def finish(row_ref, se_ref, coup_ref, heff_ref):
    slots, nstate = coup_ref.shape[1], heff_ref.shape[0]
    row = row_ref[...]
    coup_ref[...] = row[:, :slots]
    line = lax.broadcasted_iota(jnp.int32, (nstate, LANES), 0)
    lane = lax.broadcasted_iota(jnp.int32, (nstate, LANES), 1) - LANES // 2
    si = lax.broadcasted_iota(jnp.int32, (nstate, nstate), 0)
    sj = lax.broadcasted_iota(jnp.int32, (nstate, nstate), 1)
    heff = jnp.zeros((nstate, nstate), jnp.float32)
    for n in range(nstate):
        down = jnp.sum(jnp.where(lane == line * nstate + n, row, 0.0), axis=1, keepdims=True)
        up = jnp.sum(jnp.where(lane == n * nstate + line, row, 0.0), axis=1, keepdims=True)
        column = 0.5 * (down + up)
        heff = jnp.where(sj == n, column + jnp.where(si == n, se_ref[n], 0.0), heff)
    heff_ref[...] = heff


def local(
    npair,
    nvirt,
    density_row_blocks,
    vir_left,
    vir_right,
    orb_energy,
    state_energy,
    bra_ket_states,
    row_block_starts,
):
    slots, rows, ntrip = density_row_blocks.shape
    avirt = vir_left.shape[0]
    nstate = state_energy.shape[0]
    padded = -(-ntrip // LANES) * LANES
    half = -(-(ntrip + 1) // (2 * LANES)) * LANES
    hbm = pl.BlockSpec(memory_space=pltpu.HBM)
    vmem = pl.BlockSpec(memory_space=pltpu.VMEM)
    smem = pl.BlockSpec(memory_space=pltpu.SMEM)
    dma = pltpu.SemaphoreType.DMA
    nz = nvirt // 2
    cut = pl.pallas_call(
        windows,
        out_shape=(
            jax.ShapeDtypeStruct((nvirt, avirt, slots * rows), jnp.bfloat16),
            jax.ShapeDtypeStruct((2, avirt, half), jnp.bfloat16),
            jax.ShapeDtypeStruct((1, slots * rows), jnp.float32),
            jax.ShapeDtypeStruct((slots * rows, LANES), jnp.bfloat16),
        ),
        in_specs=[vmem, vmem, vmem, smem, smem, smem],
        out_specs=(vmem,) * 4,
        scratch_shapes=[pltpu.VMEM((avirt, padded + nvirt * rows), jnp.float32)],
    )(
        vir_left,
        vir_right,
        orb_energy.reshape(1, avirt),
        state_energy,
        bra_ket_states.T,
        row_block_starts,
    )
    row = pl.pallas_call(
        functools.partial(kernel, npair, nvirt),
        out_shape=jax.ShapeDtypeStruct((1, LANES), jnp.float32),
        in_specs=[hbm, vmem, vmem, vmem, vmem],
        out_specs=vmem,
        scratch_shapes=[
            pltpu.VMEM((slots, rows, ntrip), jnp.bfloat16),
            pltpu.VMEM((2, nvirt, avirt, half), jnp.bfloat16),
            pltpu.VMEM((nvirt, avirt, slots * rows), jnp.bfloat16),
            pltpu.VMEM((1, LANES), jnp.float32),
            pltpu.VMEM((nvirt, 1, LANES), jnp.float32),
            pltpu.VMEM((1, LANES), jnp.float32),
            pltpu.VMEM((npair, 1, LANES), jnp.float32),
            dma,
            dma((2,)),
            dma,
            dma((nz,)),
            dma((2,)),
            dma((nz,)),
            dma((2, nz)),
            dma((2, nvirt)),
            dma((nvirt,)),
            dma((nvirt,)),
            dma((nvirt,)),
            dma((nvirt,)),
            dma((npair,)),
            dma((npair,)),
        ],
        compiler_params=pltpu.CompilerParams(
            collective_id=0, has_side_effects=True, vmem_limit_bytes=60 * 1024 * 1024
        ),
    )(density_row_blocks, *cut)
    couplings, heff = pl.pallas_call(
        finish,
        out_shape=(
            jax.ShapeDtypeStruct((1, slots), jnp.float32),
            jax.ShapeDtypeStruct((nstate, nstate), jnp.float32),
        ),
        in_specs=[vmem, smem],
        out_specs=(vmem, vmem),
    )(row, state_energy)
    return couplings.reshape(slots), heff


def solution(mesh):
    npair, nvirt = mesh.shape["pair"], mesh.shape["virt"]
    placed = (
        P("pair", "virt", None),
        P("virt", None),
        P("virt", None),
        P("virt"),
        P(),
        P("pair", None),
        P("pair"),
    )
    return jax.shard_map(
        functools.partial(local, npair, nvirt),
        mesh=mesh,
        in_specs=placed,
        out_specs=(P("pair"), P()),
        check_vma=False,
    )
```

```python
import functools

import jax
import jax.numpy as jnp
from jax import lax
from jax.experimental import pallas as pl
from jax.experimental.pallas import tpu as pltpu
from jax.sharding import PartitionSpec as P

MESH = pl.DeviceIdType.MESH
LANES = 128


def windows(
    l_raw,
    r_raw,
    e_ref,
    se_ref,
    states_ref,
    starts_ref,
    w_send,
    r_own,
    shift_ref,
    place_ref,
    l_f32,
):
    nvirt, avirt, _ = w_send.shape
    ntrip = l_raw.shape[1]
    slots = starts_ref.shape[0]
    rows = shift_ref.shape[1] // slots
    group = LANES // rows
    blocks = slots // group

    l_f32[...] = jnp.zeros_like(l_f32)
    l_f32[:, :ntrip] = l_raw[...].astype(jnp.float32)
    lane = lax.broadcasted_iota(jnp.int32, (avirt, LANES), 1) // rows
    width = rows * nvirt
    load_width = width + LANES

    def window_block(b, carry):
        views = []
        for j in range(group):
            offset = starts_ref[b * group + j]
            rest = offset % LANES
            base = pl.multiple_of(offset - rest, LANES)
            wide = l_f32[:, pl.ds(base, load_width)]
            turned = pltpu.roll(wide, (load_width - rest) % load_width, 1)
            views.append(turned[:, :width])
        for q in range(nvirt // group):
            held = [v[:, q * LANES : (q + 1) * LANES] for v in views]
            bit = 1
            while bit < group:
                keep = (lane & bit) == 0
                fresh = list(held)
                for j in range(group):
                    if j & bit == 0:
                        a, o = held[j], held[j | bit]
                        fresh[j] = jnp.where(keep, a, pltpu.roll(o, bit * rows, 1))
                        fresh[j | bit] = jnp.where(keep, pltpu.roll(a, LANES - bit * rows, 1), o)
                held = fresh
                bit *= 2
            for i in range(group):
                w_send[q * group + i, :, pl.ds(pl.multiple_of(b * LANES, LANES), LANES)] = held[
                    i
                ].astype(jnp.bfloat16)
        return carry

    lax.fori_loop(0, blocks, window_block, 0)
    square = (
        lax.broadcasted_iota(jnp.int32, (avirt, avirt), 0)
        == lax.broadcasted_iota(jnp.int32, (avirt, avirt), 1)
    )
    energy_own = jnp.sum(
        jnp.where(square, e_ref[...].astype(jnp.float32), 0.0), axis=1, keepdims=True
    )
    half = r_own.shape[2]
    rest = ntrip - half
    r_own[0] = r_raw[:, :half]
    r_own[1] = jnp.concatenate(
        [r_raw[:, half:], jnp.broadcast_to(energy_own, (avirt, half - rest)).astype(jnp.bfloat16)],
        axis=1,
    )

    wide_lane = lax.broadcasted_iota(jnp.int32, (1, LANES), 1)
    lane_of = lax.broadcasted_iota(jnp.int32, (rows, LANES), 1)
    nstate = se_ref.shape[0]
    shifts = []
    for b in range(blocks):
        shift = jnp.zeros((1, LANES), jnp.float32)
        for j in range(group):
            s = b * group + j
            i_state, j_state = states_ref[0, s], states_ref[1, s]
            total = se_ref[i_state] + se_ref[j_state]
            shift = jnp.where(wide_lane // rows == j, total, shift)
            code = LANES // 2 + i_state * nstate + j_state
            place_ref[s * rows : (s + 1) * rows, :] = (
                ((lane_of == s) | (lane_of == code)).astype(jnp.float32).astype(jnp.bfloat16)
            )
        shifts.append(shift)
    shift_ref[...] = jnp.concatenate(shifts, axis=1)


def kernel(
    npair,
    nvirt,
    d_hbm,
    w_send,
    r_own,
    shift_ref,
    place_ref,
    out_ref,
    d_all,
    r_all,
    w_all,
    p_send,
    p_all,
    d_sem,
    o_sem,
    own_sem,
    z_ssem,
    b_ssem,
    x_ssem,
    f_ssem,
    r_rsem,
    w_ssem,
    w_rsem,
    p_ssem,
    p_rsem,
    far_sem,
):
    slots, rows, ntrip = d_all.shape
    _, _, avirt, half = r_all.shape
    rest = ntrip - half
    nz = nvirt // 2
    me = lax.axis_index("virt")
    my_pair = lax.axis_index("pair")
    my_z, my_c = me // 2, me % 2
    sibling = my_z * 2 + 1 - my_c
    mine = my_pair % 2
    partner = my_pair + 1 - 2 * mine
    z_order = sorted(range(1, nz), key=lambda d: -min(d, nz - d))

    r_copies = [
        pltpu.make_async_copy(r_own.at[h], r_all.at[h, me], o_sem.at[h]) for h in range(2)
    ]
    for copy in r_copies:
        copy.start()
    d_copy = pltpu.make_async_copy(d_hbm, d_all, d_sem)
    d_copy.start()

    barrier = pltpu.get_barrier_semaphore()
    for k in range(1, nvirt):
        pl.semaphore_signal(
            barrier, inc=1, device_id={"virt": (me + k) % nvirt}, device_id_type=MESH
        )
    for k in range(1, npair):
        pl.semaphore_signal(
            barrier, inc=1, device_id={"pair": (my_pair + k) % npair}, device_id_type=MESH
        )
    pl.semaphore_wait(barrier, nvirt + npair - 2)
    for k in range(1, npair):
        pl.semaphore_signal(
            far_sem, inc=1, device_id={"pair": (my_pair + k) % npair}, device_id_type=MESH
        )

    def send_right(h, source, device, send_sem, own=False):
        return pltpu.make_async_remote_copy(
            src_ref=r_own.at[h] if own else r_all.at[h, source],
            dst_ref=r_all.at[h, source],
            send_sem=send_sem,
            recv_sem=r_rsem.at[h, source],
            device_id=device,
            device_id_type=MESH,
        )

    sends = []

    def go(copy):
        copy.start()
        sends.append(copy)

    def same_core(dz):
        return ((my_z + dz) % nz) * 2 + my_c

    for dz in z_order:
        go(send_right(mine, me, {"virt": same_core(dz)}, z_ssem.at[dz], True))
    for h in range(2):
        go(send_right(h, me, {"virt": sibling}, b_ssem.at[h], True))
    for k in [2 * dz + o for dz in z_order for o in (0, 1)] + [1]:
        target = (me + k) % nvirt
        go(
            pltpu.make_async_remote_copy(
                src_ref=w_send.at[target],
                dst_ref=w_all.at[me],
                send_sem=w_ssem.at[k],
                recv_sem=w_rsem.at[me],
                device_id={"virt": target},
                device_id_type=MESH,
            )
        )
    own = pltpu.make_async_copy(w_send.at[me], w_all.at[me], own_sem)
    own.start()

    z_near = z_order[::-1]
    for dz in z_near:
        source = same_core(dz)
        send_right(mine, source, {"virt": sibling}, f_ssem.at[0, dz]).wait_recv()
        go(send_right(mine, source, {"pair": partner}, x_ssem.at[dz]))
        go(send_right(mine, source, {"virt": sibling}, f_ssem.at[0, dz]))
    for dz in z_near:
        source = same_core(dz)
        send_right(1 - mine, source, {"virt": sibling}, f_ssem.at[1, dz]).wait_recv()
        go(send_right(1 - mine, source, {"virt": sibling}, f_ssem.at[1, dz]))
    d_copy.wait()
    for copy in r_copies:
        copy.wait()
    for dz in range(nz):
        source = ((my_z + dz) % nz) * 2 + 1 - my_c
        for h in range(2):
            send_right(h, source, {"virt": sibling}, f_ssem.at[0, 0]).wait_recv()
    total = None
    for h, (lo, cw) in enumerate(((0, half), (half, rest))):
        part = lax.dot_general(
            r_all[h, :, :, :cw].reshape(nvirt * avirt, cw),
            d_all[:, :, lo : lo + cw].reshape(slots * rows, cw),
            (((1,), (1,)), ((), ())),
            preferred_element_type=jnp.float32,
        )
        total = part if total is None else total + part
    energy = r_all[1, :, :, half - LANES :].reshape(nvirt * avirt, LANES)[:, LANES - 1 :]
    inverse = 1.0 / (energy.astype(jnp.float32) - shift_ref[...])
    total = total * inverse
    own.wait()
    for k in range(1, nvirt):
        source = (me + k) % nvirt
        pltpu.make_async_remote_copy(
            src_ref=w_send.at[source],
            dst_ref=w_all.at[source],
            send_sem=w_ssem.at[0],
            recv_sem=w_rsem.at[source],
            device_id={"virt": source},
            device_id_type=MESH,
        ).wait_recv()
    columns = w_all[...].reshape(nvirt * avirt, slots * rows)
    summed = jnp.sum(total * columns.astype(jnp.float32), axis=0, keepdims=True)
    high = summed.astype(jnp.bfloat16).astype(jnp.float32)
    middle = (summed - high).astype(jnp.bfloat16).astype(jnp.float32)
    low = summed - high - middle
    terms = jnp.concatenate(
        [high, middle, low, jnp.zeros((5, slots * rows), jnp.float32)], axis=0
    ).astype(jnp.bfloat16)
    placed = jnp.dot(terms, place_ref[...], preferred_element_type=jnp.float32)
    partial = jnp.sum(placed, axis=0, keepdims=True)

    pl.semaphore_wait(far_sem, npair - 1)
    count = npair * nvirt
    number = my_pair * nvirt + me
    p_send[...] = partial

    def row_copy(k, own):
        other = lax.rem(number + k, count)
        return pltpu.make_async_remote_copy(
            src_ref=p_send,
            dst_ref=p_all.at[number if own else other],
            send_sem=p_ssem.at[k],
            recv_sem=p_rsem.at[number if own else other],
            device_id={"pair": lax.div(other, nvirt), "virt": lax.rem(other, nvirt)},
            device_id_type=MESH,
        )

    def send_row(k, carry):
        row_copy(k, True).start()
        return carry

    def take_row(k, carry):
        row_copy(k, False).wait_recv()
        return carry

    def end_row(k, carry):
        row_copy(k, True).wait_send()
        return carry

    lax.fori_loop(1, count, send_row, 0, unroll=count <= 64)
    p_all[number] = partial
    lax.fori_loop(1, count, take_row, 0, unroll=count <= 64)
    along = jnp.sum(p_all[pl.ds(my_pair * nvirt, nvirt)], axis=0)
    lane = lax.broadcasted_iota(jnp.int32, (1, LANES), 1)
    out_ref[...] = jnp.where(lane < LANES // 2, along, jnp.sum(p_all[...], axis=0))
    lax.fori_loop(1, count, end_row, 0, unroll=count <= 64)
    for send in sends:
        send.wait_send()


def finish(row_ref, se_ref, coup_ref, heff_ref):
    slots, nstate = coup_ref.shape[1], heff_ref.shape[0]
    row = row_ref[...]
    coup_ref[...] = row[:, :slots]
    line = lax.broadcasted_iota(jnp.int32, (nstate, LANES), 0)
    lane = lax.broadcasted_iota(jnp.int32, (nstate, LANES), 1) - LANES // 2
    si = lax.broadcasted_iota(jnp.int32, (nstate, nstate), 0)
    sj = lax.broadcasted_iota(jnp.int32, (nstate, nstate), 1)
    heff = jnp.zeros((nstate, nstate), jnp.float32)
    for n in range(nstate):
        down = jnp.sum(jnp.where(lane == line * nstate + n, row, 0.0), axis=1, keepdims=True)
        up = jnp.sum(jnp.where(lane == n * nstate + line, row, 0.0), axis=1, keepdims=True)
        column = 0.5 * (down + up)
        heff = jnp.where(sj == n, column + jnp.where(si == n, se_ref[n], 0.0), heff)
    heff_ref[...] = heff


def local(
    npair,
    nvirt,
    density_row_blocks,
    vir_left,
    vir_right,
    orb_energy,
    state_energy,
    bra_ket_states,
    row_block_starts,
):
    slots, rows, ntrip = density_row_blocks.shape
    avirt = vir_left.shape[0]
    nstate = state_energy.shape[0]
    padded = -(-ntrip // LANES) * LANES
    half = -(-(ntrip + 1) // (2 * LANES)) * LANES
    hbm = pl.BlockSpec(memory_space=pltpu.HBM)
    vmem = pl.BlockSpec(memory_space=pltpu.VMEM)
    smem = pl.BlockSpec(memory_space=pltpu.SMEM)
    dma = pltpu.SemaphoreType.DMA
    nz = nvirt // 2
    cut = pl.pallas_call(
        windows,
        out_shape=(
            jax.ShapeDtypeStruct((nvirt, avirt, slots * rows), jnp.bfloat16),
            jax.ShapeDtypeStruct((2, avirt, half), jnp.bfloat16),
            jax.ShapeDtypeStruct((1, slots * rows), jnp.float32),
            jax.ShapeDtypeStruct((slots * rows, LANES), jnp.bfloat16),
        ),
        in_specs=[vmem, vmem, vmem, smem, smem, smem],
        out_specs=(vmem,) * 4,
        scratch_shapes=[pltpu.VMEM((avirt, padded + nvirt * rows), jnp.float32)],
    )(
        vir_left,
        vir_right,
        orb_energy.reshape(1, avirt),
        state_energy,
        bra_ket_states.T,
        row_block_starts,
    )
    row = pl.pallas_call(
        functools.partial(kernel, npair, nvirt),
        out_shape=jax.ShapeDtypeStruct((1, LANES), jnp.float32),
        in_specs=[hbm, vmem, vmem, vmem, vmem],
        out_specs=vmem,
        scratch_shapes=[
            pltpu.VMEM((slots, rows, ntrip), jnp.bfloat16),
            pltpu.VMEM((2, nvirt, avirt, half), jnp.bfloat16),
            pltpu.VMEM((nvirt, avirt, slots * rows), jnp.bfloat16),
            pltpu.VMEM((1, LANES), jnp.float32),
            pltpu.VMEM((npair * nvirt, 1, LANES), jnp.float32),
            dma,
            dma((2,)),
            dma,
            dma((nz,)),
            dma((2,)),
            dma((nz,)),
            dma((2, nz)),
            dma((2, nvirt)),
            dma((nvirt,)),
            dma((nvirt,)),
            dma((npair * nvirt,)),
            dma((npair * nvirt,)),
            pltpu.SemaphoreType.REGULAR,
        ],
        compiler_params=pltpu.CompilerParams(
            collective_id=0, has_side_effects=True, vmem_limit_bytes=60 * 1024 * 1024
        ),
    )(density_row_blocks, *cut)
    couplings, heff = pl.pallas_call(
        finish,
        out_shape=(
            jax.ShapeDtypeStruct((1, slots), jnp.float32),
            jax.ShapeDtypeStruct((nstate, nstate), jnp.float32),
        ),
        in_specs=[vmem, smem],
        out_specs=(vmem, vmem),
    )(row, state_energy)
    return couplings.reshape(slots), heff


def solution(mesh):
    npair, nvirt = mesh.shape["pair"], mesh.shape["virt"]
    placed = (
        P("pair", "virt", None),
        P("virt", None),
        P("virt", None),
        P("virt"),
        P(),
        P("pair", None),
        P("pair"),
    )
    return jax.shard_map(
        functools.partial(local, npair, nvirt),
        mesh=mesh,
        in_specs=placed,
        out_specs=(P("pair"), P()),
        check_vma=False,
    )
```
